32 devices in a mesh: rep: 2 (over y), seq: 4 (over z), tp: 4 (over x, core).
Axes of the slice: x: 2, y: 2, z: 4, core: 2. Of those that a mesh axis runs over, the one named last changes fastest.
Arguments:
- queries: bfloat16 [128, 64, 128], P(('rep', 'seq')), parts along dimension 0, may hold values from -9 to 9
- key_pages: bfloat16 [1024, 8, 64, 128], P(('rep', 'seq'), 'tp'), parts along dimension 0, may hold values from -4 to 4
- value_pages: bfloat16 [1024, 8, 64, 128], P(('rep', 'seq'), 'tp'), parts along dimension 0, may hold values from -6 to 6
- page_owner: int32 [128, 128], P('rep'), parts along dimension 0, may hold values from 0 to 3, as said below
- page_local: int32 [128, 128], P('rep'), parts along dimension 0, may hold values from 0 to 127, as said below
- seq_lengths: int32 [128], P('rep'), parts along dimension 0, may hold values from 1 to 8192, as said below
Outputs:
- attention: bfloat16 [128, 64, 128], P(('rep', 'seq'), 'tp'), parts along dimension 0
The draws below stay inside these ranges and needn't reach their ends.
There are 2 independent parts, one for each index of `rep`. The reference program is written for one: setup_inputs(seed, part) draws one part's arguments, and reference() takes and returns one part's arrays. A program takes and returns all parts, laid end to end along the dimension named above; each array names one. Nothing has to cross between parts.
Inputs may be any that keep to these rules, and one draw needn't show every extreme that they name: The live slots (s * 64 < seq_lengths[b]) name pairs (page_owner, page_local) that are all different; the other slots hold 0. `page_local`: see page_owner. `seq_lengths`: one sequence has exactly 8192 tokens; the live slots of all sequences together number at most half of the 512 pages.
All inputs are finite; a program needn't handle non-finite values.
Results may differ from the reference program's by a relative error of at most 0.008.
Values may be sent and summed in bfloat16 or wider, within the bound.
A program may use at most 64 MiB of HBM per device.

```python
import math
import jax
import jax.numpy as jnp
from jax import lax

HQ = 64
KVH = 8
HD = 128
PAGE = 64
SEQS = 64
P_DEV = 128
POOL = 512
MAXP = 128
N_SEQ = 4


def page_layout(key):
    base = jax.random.fold_in(key, 7)
    keys_list = jax.random.split(base, 5)
    longest = jax.random.randint(keys_list[0], (), 0, SEQS)
    upper = max(1, POOL // (4 * (SEQS - 1)))
    seq_index = jnp.arange(SEQS, dtype=jnp.int32)
    page_count = jax.random.randint(keys_list[1], (SEQS,), 1, upper + 1)
    page_count = jnp.where(seq_index == longest, MAXP, page_count).astype(jnp.int32)
    last_fill = jax.random.randint(keys_list[2], (SEQS,), 1, PAGE + 1)
    last_fill = jnp.where(seq_index == longest, PAGE, last_fill).astype(jnp.int32)
    lengths = (page_count - 1) * PAGE + last_fill
    slot_ids = jnp.arange(MAXP, dtype=jnp.int32)
    used = (slot_ids[None, :] < page_count[:, None]).reshape(-1).astype(jnp.int32)
    ordinal = jnp.cumsum(used) - 1
    device_weight = jax.random.randint(keys_list[3], (N_SEQ,), 1, 17)
    raw_score = jax.random.randint(keys_list[4], (POOL,), 0, 65536)
    pool_ids = jnp.arange(POOL, dtype=jnp.int32)
    score = raw_score // device_weight[pool_ids // P_DEV] * POOL + pool_ids
    pool_order = jnp.argsort(score).astype(jnp.int32)
    target = pool_order[jnp.clip(ordinal, 0, POOL - 1)]
    target = jnp.where(used > 0, target, 0).reshape(SEQS, MAXP)
    return (lengths.astype(jnp.int32), (target // P_DEV).astype(jnp.int32), (target % P_DEV).astype(jnp.int32))


def draw_seq_lengths(key, part):
    return page_layout(key)[0]


def draw_page_owner(key, part):
    return page_layout(key)[1]


def draw_page_local(key, part):
    return page_layout(key)[2]


def draw_queries(key, part):
    values = jax.random.truncated_normal(key, -4.0, 4.0, (SEQS, HQ, HD), jnp.float32)
    row_scale = jnp.exp(jax.random.uniform(jax.random.fold_in(key, 3), (SEQS, 1, 1), jnp.float32, -0.7, 0.7))
    return (values * row_scale).astype(jnp.bfloat16)


def block_levels(key, dims, cuts, smallest, top_value):
    gain = 1.0
    for axis_at, parts in cuts:
        draws = jax.random.uniform(jax.random.fold_in(jax.random.fold_in(key, 6), axis_at), (parts,), jnp.float32, smallest / len(cuts), top_value / len(cuts))
        gain = gain * jnp.repeat(jnp.exp(draws), dims[axis_at] // parts).reshape((-1,) + (1,) * (len(dims) - 1 - axis_at))
    return gain


def bell_draw(rng, extent, scale, most, cuts=(), kind=jnp.bfloat16):
    loudness = block_levels(rng, extent, cuts, -0.22, 0.18) if cuts else 1.0
    values = jax.random.normal(rng, extent, jnp.float32) * scale * loudness
    return jnp.minimum(jnp.maximum(values, -most), most).astype(kind)


def setup_inputs(seed: int = 0, part: int = 0) -> dict:
    arg_keys = jax.random.split(jax.random.key(seed), 7)
    own_keys = jax.random.split(jax.random.fold_in(arg_keys[6], part), 7)
    queries = draw_queries(jax.random.fold_in(jax.random.fold_in(arg_keys[6], part), 71), part)
    key_pages = bell_draw(own_keys[1], (POOL, KVH, PAGE, HD), 1.0, 4.0, ((0, 4), (1, 4)))
    value_pages = bell_draw(own_keys[2], (POOL, KVH, PAGE, HD), 1.0, 6.0, ((0, 4), (1, 4)))
    page_owner = draw_page_owner(jax.random.fold_in(jax.random.fold_in(arg_keys[6], part), 71), part)
    page_local = draw_page_local(jax.random.fold_in(jax.random.fold_in(arg_keys[6], part), 71), part)
    seq_lengths = draw_seq_lengths(jax.random.fold_in(jax.random.fold_in(arg_keys[6], part), 71), part)
    return dict(queries=queries, key_pages=key_pages, value_pages=value_pages, page_owner=page_owner, page_local=page_local, seq_lengths=seq_lengths)


score_shift = 8.0

def reference(queries, key_pages, value_pages, page_owner, page_local, seq_lengths):
    group_size = HQ // KVH
    slot_ids = jnp.arange(MAXP, dtype=jnp.int32)
    slot_fill = jnp.clip(seq_lengths[:, None] - slot_ids[None, :] * PAGE, 0, PAGE).astype(jnp.int32)
    pool_index = (page_owner * P_DEV + page_local).astype(jnp.int32)
    target = jnp.where(slot_fill > 0, pool_index, POOL).astype(jnp.int32).reshape(-1)
    seq_ids = jnp.broadcast_to(jnp.arange(SEQS, dtype=jnp.int32)[:, None], (SEQS, MAXP)).reshape(-1)
    page_seq = jnp.zeros((POOL,), jnp.int32).at[target].set(seq_ids, mode='drop')
    page_fill = jnp.zeros((POOL,), jnp.int32).at[target].set(slot_fill.reshape(-1), mode='drop')
    block_pages = math.gcd(POOL, 64)
    block_count = POOL // block_pages
    key_blocks = key_pages.reshape(block_count, block_pages, KVH, PAGE, HD)
    value_blocks = value_pages.reshape(block_count, block_pages, KVH, PAGE, HD)
    seq_blocks = page_seq.reshape(block_count, block_pages)
    fill_blocks = page_fill.reshape(block_count, block_pages)
    score_scale = 1.0 / math.sqrt(HD)

    def visit(carry, block):
        numerator, denominator = carry
        key_block, value_block, seq_block, fill_block = block
        picked = queries[seq_block].astype(jnp.float32).reshape(block_pages, KVH, group_size, HD)
        scores = jnp.einsum('pkgd,pktd->pkgt', picked, key_block.astype(jnp.float32), precision=lax.Precision.HIGHEST) * score_scale
        live_mask = jnp.arange(PAGE, dtype=jnp.int32)[None, :] < fill_block[:, None]
        weight = jnp.where(live_mask[:, None, None, :], jnp.exp(scores - score_shift), 0.0)
        page_total = lax.optimization_barrier(jnp.sum(weight, axis=-1))
        rounded = lax.optimization_barrier(weight.astype(jnp.bfloat16)).astype(jnp.float32)
        page_sum = jnp.einsum('pkgt,pktd->pkgd', rounded, value_block.astype(jnp.float32), precision=lax.Precision.HIGHEST)
        numerator = numerator + jax.ops.segment_sum(page_sum, seq_block, num_segments=SEQS)
        denominator = denominator + jax.ops.segment_sum(page_total, seq_block, num_segments=SEQS)
        return ((numerator, denominator), None)
    start = (jnp.zeros((SEQS, KVH, group_size, HD), jnp.float32), jnp.zeros((SEQS, KVH, group_size), jnp.float32))
    (numerator, denominator), _ = lax.scan(visit, start, (key_blocks, value_blocks, seq_blocks, fill_blocks))
    result = numerator / denominator[..., None]
    return result.reshape(SEQS, HQ, HD).astype(jnp.bfloat16)
```

```python
import functools
import math

import jax
import jax.numpy as jnp
from jax import lax
from jax.experimental import pallas as pl
from jax.experimental.pallas import tpu as pltpu
from jax.sharding import PartitionSpec as P

HQ = 64
KVH = 8
LANES = 128
BLOCK = 8
MESH = pl.DeviceIdType.MESH

score_shift = 8.0


def kernel(
    n, q_hbm, k_hbm, v_hbm, owner_hbm, local_hbm, lens, out_ref,
    kbuf, vbuf, owner, local, qg, qf, qp, fills, onehot, spread, pages, tots, stage, sbuf, rbuf, outf,
    load_sem, qload_sem, kv_sem, qsend_sem, qrecv_sem, osend_sem, orecv_sem,
):
    me = lax.axis_index("seq")
    tp = lax.axis_index("tp")
    pool, kv_local, page_len, dim = k_hbm.shape
    seqs, slots = owner_hbm.shape
    group = HQ // KVH
    rows = seqs // n
    bits = page_len.bit_length()
    scale = 1.0 / math.sqrt(dim)

    table_loads = []
    for at in range(0, slots, LANES):
        part = at // LANES
        for i, (src, dst) in enumerate(((owner_hbm, owner), (local_hbm, local))):
            c = pltpu.make_async_copy(src.at[:, pl.ds(at, LANES)], dst.at[part], load_sem.at[i, part])
            c.start()
            table_loads.append(c)
    q_loads = []
    for kv in range(kv_local):
        first = pl.multiple_of((tp * kv_local + kv) * group, group)
        c = pltpu.make_async_copy(q_hbm.at[:, pl.ds(first, group), :], qg.at[kv, me], qload_sem.at[kv])
        c.start()
        q_loads.append(c)
    kv_loads = []
    for kv in range(kv_local):
        ck = pltpu.make_async_copy(k_hbm.at[:, kv], kbuf.at[kv], kv_sem.at[0, kv])
        cv = pltpu.make_async_copy(v_hbm.at[:, kv], vbuf.at[kv], kv_sem.at[1, kv])
        ck.start()
        cv.start()
        kv_loads.append((ck, cv))

    barrier = pltpu.get_barrier_semaphore()
    for off in range(1, n):
        pl.semaphore_signal(barrier, inc=1, device_id={"seq": lax.rem(me + off, n)}, device_id_type=MESH)
    for c in q_loads:
        c.wait()
    pl.semaphore_wait(barrier, n - 1)

    q_sends = []
    for kv in range(kv_local):
        for off in range(1, n):
            c = pltpu.make_async_remote_copy(
                src_ref=qg.at[kv, me],
                dst_ref=qg.at[kv, me],
                send_sem=qsend_sem.at[kv, off],
                recv_sem=qrecv_sem.at[kv, off],
                device_id={"seq": lax.rem(me + off, n)},
                device_id_type=MESH,
            )
            c.start()
            q_sends.append(c)

    for c in table_loads:
        c.wait()
    page_ids = lax.broadcasted_iota(jnp.int32, (pool, LANES), 0)
    lane = lax.broadcasted_iota(jnp.int32, (1, LANES), 1)

    def match(b, acc):
        length = lens[b]
        for at in range(0, slots, LANES):
            own = owner[at // LANES, pl.ds(b, 1), :]
            loc = local[at // LANES, pl.ds(b, 1), :]
            fill = jnp.clip(length - (lane + at) * page_len, 0, page_len)
            code = jnp.where((own == me) & (fill > 0), loc, -1)
            acc = jnp.where(page_ids == code, (b << bits) + fill, acc)
        return acc

    acc = lax.fori_loop(0, seqs, match, jnp.zeros((pool, LANES), jnp.int32), unroll=8)
    code = jnp.max(acc.astype(jnp.float32), axis=1, keepdims=True)
    wide = jnp.broadcast_to(code, (pool, pool))
    tall = jnp.transpose(wide)[:seqs].astype(jnp.int32)
    wide = wide.astype(jnp.int32)
    full = jnp.broadcast_to(wide[:, :1], (pool, LANES)) & ((1 << bits) - 1)
    for g in range(group):
        fills[pl.ds(g, pool, stride=group), :] = full
    seq_wide = wide[:, :seqs]
    onehot[...] = jnp.where(
        (seq_wide > 0) & ((seq_wide >> bits) == lax.broadcasted_iota(jnp.int32, (pool, seqs), 1)), 1.0, 0.0
    ).astype(jnp.bfloat16)
    spread[...] = jnp.where(
        (tall > 0) & ((tall >> bits) == lax.broadcasted_iota(jnp.int32, (seqs, pool), 0)), 1.0, 0.0
    ).astype(jnp.bfloat16)

    pair = 2 * group
    span = 2 * page_len
    row = lax.broadcasted_iota(jnp.int32, (pair, span), 0)
    col = lax.broadcasted_iota(jnp.int32, (pair, span), 1)
    token = jnp.where((row < group) == (col < page_len), jnp.where(col < page_len, col, col - page_len), span)
    row_l = lax.broadcasted_iota(jnp.int32, (pair, LANES), 0)
    col_l = lax.broadcasted_iota(jnp.int32, (pair, LANES), 1)
    head_of = jnp.where(row_l < group, row_l, row_l - group)
    spot = (col_l == head_of) | (col_l == head_of + group)

    def recv(sem, kv, off, ref):
        src = lax.rem(me + n - off, n)
        return pltpu.make_async_remote_copy(
            src_ref=ref.at[kv, src], dst_ref=ref.at[kv, src], send_sem=qsend_sem.at[kv, off],
            recv_sem=sem.at[kv, off], device_id={"seq": src}, device_id_type=MESH,
        )

    o_sends = []
    for kv in range(kv_local):
        for off in range(1, n):
            recv(qrecv_sem, kv, off, qg).wait_recv()
        qf[...] = qg[kv].reshape(seqs * group, dim).astype(jnp.float32)
        for g in range(group):
            mine = qf[pl.ds(g, seqs, stride=group), :].astype(jnp.bfloat16)
            qp[pl.ds(g, pool, stride=group), :] = jnp.dot(
                onehot[...], mine, preferred_element_type=jnp.float32
            )
        for c in kv_loads[kv]:
            c.wait()

        def attend(step, carry):
            for i in range(BLOCK):
                at = step * BLOCK + i
                rows_at = pl.ds(pl.multiple_of(at * pair, pair), pair)
                pages_at = pl.ds(at * 2, 2)
                q = qp[rows_at, :].astype(jnp.bfloat16)
                k = kbuf[kv, pages_at].reshape(span, dim)
                v = vbuf[kv, pages_at].reshape(span, dim)
                s = lax.dot_general(q, k, (((1,), (1,)), ((), ())), preferred_element_type=jnp.float32)
                w = jnp.where(token < fills[rows_at, :], jnp.exp(s * scale - score_shift), 0.0)
                total = jnp.sum(w, axis=1, keepdims=True)
                tots[rows_at, :] = jnp.where(spot, total, 0.0)
                pages[rows_at, :] = jnp.dot(w.astype(jnp.bfloat16), v, preferred_element_type=jnp.float32)
            return carry

        lax.fori_loop(0, pool // (2 * BLOCK), attend, 0)

        def collect(value):
            high = value.astype(jnp.bfloat16)
            low = (value - high.astype(jnp.float32)).astype(jnp.bfloat16)
            return jnp.dot(spread[...], high, preferred_element_type=jnp.float32) + jnp.dot(
                spread[...], low, preferred_element_type=jnp.float32
            )

        page_tot = tots[pl.ds(0, pool, stride=group), :]
        for g in range(1, group):
            page_tot += tots[pl.ds(g, pool, stride=group), :]
        tot = collect(page_tot)
        high = tot.astype(jnp.bfloat16).astype(jnp.float32)
        lanes = lax.broadcasted_iota(jnp.int32, (seqs, LANES), 1)
        tot = jnp.where(lanes < group, high, tot - high)
        for d in range(n):
            stage[kv, d, group * rows : (group + 1) * rows, :] = tot[d * rows : (d + 1) * rows]
        for g in range(group):
            num = collect(pages[pl.ds(g, pool, stride=group), :])
            for d in range(n):
                stage[kv, d, g * rows : (g + 1) * rows, :] = num[d * rows : (d + 1) * rows]
        for d in range(n):
            sbuf[kv, d] = stage[kv, d].astype(jnp.bfloat16)
        for off in range(1, n):
            peer = lax.rem(me + off, n)
            c = pltpu.make_async_remote_copy(
                src_ref=sbuf.at[kv, peer],
                dst_ref=rbuf.at[kv, me],
                send_sem=osend_sem.at[kv, off],
                recv_sem=orecv_sem.at[kv, off],
                device_id={"seq": peer},
                device_id_type=MESH,
            )
            c.start()
            o_sends.append(c)

    for kv in range(kv_local):
        whole = stage[kv, me]
        for off in range(1, n):
            recv(orecv_sem, kv, off, rbuf).wait_recv()
            whole += rbuf[kv, lax.rem(me + n - off, n)].astype(jnp.float32)
        tot = whole[group * rows :]
        for g in range(group):
            den = tot[:, g : g + 1] + tot[:, group + g : group + g + 1]
            outf[pl.ds(kv * group + g, rows, stride=kv_local * group), :] = whole[g * rows : (g + 1) * rows] / den
    out_ref[...] = outf[...].reshape(rows, kv_local * group, dim).astype(jnp.bfloat16)
    for c in q_sends:
        c.wait_send()
    for c in o_sends:
        c.wait_send()


def solution(mesh):
    n = mesh.shape["seq"]

    def body(queries, key_pages, value_pages, page_owner, page_local, seq_lengths):
        pool, kv_local, page_len, dim = key_pages.shape
        seqs, slots = page_owner.shape
        group = HQ // KVH
        rows = seqs // n
        heads = kv_local * group
        part = (group + 1) * rows
        bf16, f32 = jnp.bfloat16, jnp.float32
        anywhere = pl.BlockSpec(memory_space=pl.ANY)
        return pl.pallas_call(
            functools.partial(kernel, n),
            out_shape=jax.ShapeDtypeStruct((rows, heads, dim), bf16),
            in_specs=[anywhere] * 5 + [pl.BlockSpec(memory_space=pltpu.SMEM)],
            out_specs=pl.BlockSpec(memory_space=pltpu.VMEM),
            scratch_shapes=[
                pltpu.VMEM((kv_local, pool, page_len, dim), bf16),
                pltpu.VMEM((kv_local, pool, page_len, dim), bf16),
                pltpu.VMEM((slots // LANES, seqs, LANES), jnp.int32),
                pltpu.VMEM((slots // LANES, seqs, LANES), jnp.int32),
                pltpu.VMEM((kv_local, n, rows, group, dim), bf16),
                pltpu.VMEM((seqs * group, dim), f32),
                pltpu.VMEM((pool * group, dim), f32),
                pltpu.VMEM((pool * group, LANES), jnp.int32),
                pltpu.VMEM((pool, seqs), bf16),
                pltpu.VMEM((seqs, pool), bf16),
                pltpu.VMEM((pool * group, dim), f32),
                pltpu.VMEM((pool * group, LANES), f32),
                pltpu.VMEM((kv_local, n, part, dim), f32),
                pltpu.VMEM((kv_local, n, part, dim), bf16),
                pltpu.VMEM((kv_local, n, part, dim), bf16),
                pltpu.VMEM((rows * heads, dim), f32),
                pltpu.SemaphoreType.DMA((2, slots // LANES)),
                pltpu.SemaphoreType.DMA((kv_local,)),
                pltpu.SemaphoreType.DMA((2, kv_local)),
                pltpu.SemaphoreType.DMA((kv_local, n)),
                pltpu.SemaphoreType.DMA((kv_local, n)),
                pltpu.SemaphoreType.DMA((kv_local, n)),
                pltpu.SemaphoreType.DMA((kv_local, n)),
            ],
            compiler_params=pltpu.CompilerParams(
                collective_id=0, has_side_effects=True, vmem_limit_bytes=48 * 1024 * 1024
            ),
        )(queries, key_pages, value_pages, page_owner, page_local, seq_lengths)

    placed = (
        P(("rep", "seq"), None, None),
        P(("rep", "seq"), "tp", None, None),
        P(("rep", "seq"), "tp", None, None),
        P("rep", None),
        P("rep", None),
        P("rep"),
    )
    return jax.shard_map(
        body, mesh=mesh, in_specs=placed, out_specs=P(("rep", "seq"), "tp", None), check_vma=False
    )
```

```python
import functools
import math

import jax
import jax.numpy as jnp
from jax import lax
from jax.experimental import pallas as pl
from jax.experimental.pallas import tpu as pltpu
from jax.sharding import PartitionSpec as P

HQ = 64
KVH = 8
LANES = 128
BLOCK = 8
MESH = pl.DeviceIdType.MESH

score_shift = 8.0


def kernel(
    n, q_hbm, k_hbm, v_hbm, owner_hbm, local_hbm, lens, out_ref,
    kbuf, vbuf, owner, local, qg, qf, qp, fills, onehot, spread, pages, tots, stage, sbuf, rbuf, outf,
    load_sem, qload_sem, kv_sem, qsend_sem, qrecv_sem, osend_sem, orecv_sem,
):
    me = lax.axis_index("seq")
    tp = lax.axis_index("tp")
    pool, kv_local, page_len, dim = k_hbm.shape
    seqs, slots = owner_hbm.shape
    group = HQ // KVH
    rows = seqs // n
    bits = page_len.bit_length()
    scale = 1.0 / math.sqrt(dim)

    table_loads = []
    for at in range(0, slots, LANES):
        part = at // LANES
        for i, (src, dst) in enumerate(((owner_hbm, owner), (local_hbm, local))):
            c = pltpu.make_async_copy(src.at[:, pl.ds(at, LANES)], dst.at[part], load_sem.at[i, part])
            c.start()
            table_loads.append(c)
    q_loads = []
    for kv in range(kv_local):
        first = pl.multiple_of((tp * kv_local + kv) * group, group)
        c = pltpu.make_async_copy(q_hbm.at[:, pl.ds(first, group), :], qg.at[kv, me], qload_sem.at[kv])
        c.start()
        q_loads.append(c)
    kv_loads = []
    for kv in range(kv_local):
        ck = pltpu.make_async_copy(k_hbm.at[:, kv], kbuf.at[kv], kv_sem.at[0, kv])
        cv = pltpu.make_async_copy(v_hbm.at[:, kv], vbuf.at[kv], kv_sem.at[1, kv])
        ck.start()
        cv.start()
        kv_loads.append((ck, cv))

    barrier = pltpu.get_barrier_semaphore()
    for off in range(1, n):
        pl.semaphore_signal(barrier, inc=1, device_id={"seq": lax.rem(me + off, n)}, device_id_type=MESH)
    for c in q_loads:
        c.wait()
    pl.semaphore_wait(barrier, n - 1)

    q_sends = []
    for kv in range(kv_local):
        for off in range(1, n):
            c = pltpu.make_async_remote_copy(
                src_ref=qg.at[kv, me],
                dst_ref=qg.at[kv, me],
                send_sem=qsend_sem.at[kv, off],
                recv_sem=qrecv_sem.at[kv, off],
                device_id={"seq": lax.rem(me + off, n)},
                device_id_type=MESH,
            )
            c.start()
            q_sends.append(c)

    for c in table_loads:
        c.wait()
    page_ids = lax.broadcasted_iota(jnp.int32, (pool, LANES), 0)
    lane = lax.broadcasted_iota(jnp.int32, (1, LANES), 1)

    def match(b, acc):
        length = lens[b]
        for at in range(0, slots, LANES):
            own = owner[at // LANES, pl.ds(b, 1), :]
            loc = local[at // LANES, pl.ds(b, 1), :]
            fill = jnp.clip(length - (lane + at) * page_len, 0, page_len)
            code = jnp.where((own == me) & (fill > 0), loc, -1)
            acc = jnp.where(page_ids == code, (b << bits) + fill, acc)
        return acc

    acc = lax.fori_loop(0, seqs, match, jnp.zeros((pool, LANES), jnp.int32), unroll=8)
    code = jnp.max(acc.astype(jnp.float32), axis=1, keepdims=True)
    wide = jnp.broadcast_to(code, (pool, pool))
    tall = jnp.transpose(wide)[:seqs].astype(jnp.int32)
    wide = wide.astype(jnp.int32)
    full = jnp.broadcast_to(wide[:, :1], (pool, LANES)) & ((1 << bits) - 1)
    for g in range(group):
        fills[pl.ds(g, pool, stride=group), :] = full
    seq_wide = wide[:, :seqs]
    onehot[...] = jnp.where(
        (seq_wide > 0) & ((seq_wide >> bits) == lax.broadcasted_iota(jnp.int32, (pool, seqs), 1)), 1.0, 0.0
    ).astype(jnp.bfloat16)
    spread[...] = jnp.where(
        (tall > 0) & ((tall >> bits) == lax.broadcasted_iota(jnp.int32, (seqs, pool), 0)), 1.0, 0.0
    ).astype(jnp.bfloat16)

    pair = 2 * group
    span = 2 * page_len
    row = lax.broadcasted_iota(jnp.int32, (pair, span), 0)
    col = lax.broadcasted_iota(jnp.int32, (pair, span), 1)
    token = jnp.where((row < group) == (col < page_len), jnp.where(col < page_len, col, col - page_len), span)
    row_l = lax.broadcasted_iota(jnp.int32, (pair, LANES), 0)
    col_l = lax.broadcasted_iota(jnp.int32, (pair, LANES), 1)
    head_of = jnp.where(row_l < group, row_l, row_l - group)
    spot = (col_l == head_of) | (col_l == head_of + group)

    def recv(sem, kv, off, ref):
        src = lax.rem(me + n - off, n)
        return pltpu.make_async_remote_copy(
            src_ref=ref.at[kv, src], dst_ref=ref.at[kv, src], send_sem=qsend_sem.at[kv, off],
            recv_sem=sem.at[kv, off], device_id={"seq": src}, device_id_type=MESH,
        )

    o_sends = []
    for kv in range(kv_local):
        for off in range(1, n):
            recv(qrecv_sem, kv, off, qg).wait_recv()
        qf[...] = qg[kv].reshape(seqs * group, dim).astype(jnp.float32)
        for g in range(group):
            mine = qf[pl.ds(g, seqs, stride=group), :].astype(jnp.bfloat16)
            qp[pl.ds(g, pool, stride=group), :] = jnp.dot(
                onehot[...], mine, preferred_element_type=jnp.float32
            )
        for c in kv_loads[kv]:
            c.wait()

        def attend(step, carry):
            for i in range(BLOCK):
                at = step * BLOCK + i
                rows_at = pl.ds(pl.multiple_of(at * pair, pair), pair)
                pages_at = pl.ds(at * 2, 2)
                q = qp[rows_at, :].astype(jnp.bfloat16)
                k = kbuf[kv, pages_at].reshape(span, dim)
                v = vbuf[kv, pages_at].reshape(span, dim)
                s = lax.dot_general(q, k, (((1,), (1,)), ((), ())), preferred_element_type=jnp.float32)
                w = jnp.where(token < fills[rows_at, :], jnp.exp(s * scale - score_shift), 0.0)
                total = jnp.sum(w, axis=1, keepdims=True)
                tots[rows_at, :] = jnp.where(spot, total, 0.0)
                pages[rows_at, :] = jnp.dot(w.astype(jnp.bfloat16), v, preferred_element_type=jnp.float32)
            return carry

        lax.fori_loop(0, pool // (2 * BLOCK), attend, 0)

        def collect(value):
            high = value.astype(jnp.bfloat16)
            low = (value - high.astype(jnp.float32)).astype(jnp.bfloat16)
            return jnp.dot(spread[...], high, preferred_element_type=jnp.float32) + jnp.dot(
                spread[...], low, preferred_element_type=jnp.float32
            )

        page_tot = tots[pl.ds(0, pool, stride=group), :]
        for g in range(1, group):
            page_tot += tots[pl.ds(g, pool, stride=group), :]
        tot = collect(page_tot)
        high = tot.astype(jnp.bfloat16).astype(jnp.float32)
        lanes = lax.broadcasted_iota(jnp.int32, (seqs, LANES), 1)
        tot = jnp.where(lanes < group, high, tot - high)
        for d in range(n):
            stage[kv, d, group * rows : (group + 1) * rows, :] = tot[d * rows : (d + 1) * rows]
        for g in range(group):
            num = collect(pages[pl.ds(g, pool, stride=group), :])
            for d in range(n):
                stage[kv, d, g * rows : (g + 1) * rows, :] = num[d * rows : (d + 1) * rows]
        for d in range(n):
            sbuf[kv, d] = stage[kv, d].astype(jnp.bfloat16)
        for off in range(1, n):
            peer = lax.rem(me + off, n)
            c = pltpu.make_async_remote_copy(
                src_ref=sbuf.at[kv, peer],
                dst_ref=rbuf.at[kv, me],
                send_sem=osend_sem.at[kv, off],
                recv_sem=orecv_sem.at[kv, off],
                device_id={"seq": peer},
                device_id_type=MESH,
            )
            c.start()
            o_sends.append(c)

    for kv in range(kv_local):
        whole = stage[kv, me]
        for off in range(1, n):
            recv(orecv_sem, kv, off, rbuf).wait_recv()
            whole += rbuf[kv, lax.rem(me + n - off, n)].astype(jnp.float32)
        tot = whole[group * rows :]
        for g in range(group):
            den = tot[:, g : g + 1] + tot[:, group + g : group + g + 1]
            outf[pl.ds(kv * group + g, rows, stride=kv_local * group), :] = whole[g * rows : (g + 1) * rows] / den
    out_ref[...] = outf[...].reshape(rows, kv_local * group, dim).astype(jnp.bfloat16)
    for c in q_sends:
        c.wait_send()
    for c in o_sends:
        c.wait_send()


def solution(mesh):
    n = mesh.shape["seq"]

    def body(queries, key_pages, value_pages, page_owner, page_local, seq_lengths):
        pool, kv_local, page_len, dim = key_pages.shape
        seqs, slots = page_owner.shape
        group = HQ // KVH
        rows = seqs // n
        heads = kv_local * group
        part = (group + 1) * rows
        bf16, f32 = jnp.bfloat16, jnp.float32
        in_hbm = pl.BlockSpec(memory_space=pltpu.HBM)
        return pl.pallas_call(
            functools.partial(kernel, n),
            out_shape=jax.ShapeDtypeStruct((rows, heads, dim), bf16),
            in_specs=[in_hbm] * 5 + [pl.BlockSpec(memory_space=pltpu.SMEM)],
            out_specs=pl.BlockSpec(memory_space=pltpu.VMEM),
            scratch_shapes=[
                pltpu.VMEM((kv_local, pool, page_len, dim), bf16),
                pltpu.VMEM((kv_local, pool, page_len, dim), bf16),
                pltpu.VMEM((slots // LANES, seqs, LANES), jnp.int32),
                pltpu.VMEM((slots // LANES, seqs, LANES), jnp.int32),
                pltpu.VMEM((kv_local, n, rows, group, dim), bf16),
                pltpu.VMEM((seqs * group, dim), f32),
                pltpu.VMEM((pool * group, dim), f32),
                pltpu.VMEM((pool * group, LANES), jnp.int32),
                pltpu.VMEM((pool, seqs), bf16),
                pltpu.VMEM((seqs, pool), bf16),
                pltpu.VMEM((pool * group, dim), f32),
                pltpu.VMEM((pool * group, LANES), f32),
                pltpu.VMEM((kv_local, n, part, dim), f32),
                pltpu.VMEM((kv_local, n, part, dim), bf16),
                pltpu.VMEM((kv_local, n, part, dim), bf16),
                pltpu.VMEM((rows * heads, dim), f32),
                pltpu.SemaphoreType.DMA((2, slots // LANES)),
                pltpu.SemaphoreType.DMA((kv_local,)),
                pltpu.SemaphoreType.DMA((2, kv_local)),
                pltpu.SemaphoreType.DMA((kv_local, n)),
                pltpu.SemaphoreType.DMA((kv_local, n)),
                pltpu.SemaphoreType.DMA((kv_local, n)),
                pltpu.SemaphoreType.DMA((kv_local, n)),
            ],
            compiler_params=pltpu.CompilerParams(
                collective_id=0, has_side_effects=True, vmem_limit_bytes=67043328
            ),
        )(queries, key_pages, value_pages, page_owner, page_local, seq_lengths)

    placed = (
        P(("rep", "seq"), None, None),
        P(("rep", "seq"), "tp", None, None),
        P(("rep", "seq"), "tp", None, None),
        P("rep", None),
        P("rep", None),
        P("rep"),
    )
    return jax.shard_map(
        body, mesh=mesh, in_specs=placed, out_specs=P(("rep", "seq"), "tp", None), check_vma=False
    )
```

```python
import functools
import math

import jax
import jax.numpy as jnp
from jax import lax
from jax.experimental import pallas as pl
from jax.experimental.pallas import tpu as pltpu
from jax.sharding import PartitionSpec as P

HQ = 64
KVH = 8
LANES = 128
QUAD = 4
MESH = pl.DeviceIdType.MESH

score_shift = 8.0


def kernel(
    n, q_hbm, k_hbm, v_hbm, owner_hbm, local_hbm, lens, out_ref,
    kbuf, vbuf, owner, local, qg, qf, qp, fills, codes, onehot, spread, pages, stage, sbuf, rbuf, outf,
    load_sem, qload_sem, kv_sem, qsend_sem, qrecv_sem, osend_sem, orecv_sem,
):
    me = lax.axis_index("seq")
    tp = lax.axis_index("tp")
    pool, kv_local, page_len, dim = k_hbm.shape
    seqs, slots = owner_hbm.shape
    group = HQ // KVH
    rows = seqs // n
    bits = page_len.bit_length()
    scale = 1.0 / math.sqrt(dim)

    table_loads = []
    for at in range(0, slots, LANES):
        part = at // LANES
        for i, (src, dst) in enumerate(((owner_hbm, owner), (local_hbm, local))):
            c = pltpu.make_async_copy(src.at[:, pl.ds(at, LANES)], dst.at[part], load_sem.at[i, part])
            c.start()
            table_loads.append(c)
    q_loads = []
    for kv in range(kv_local):
        first = pl.multiple_of((tp * kv_local + kv) * group, group)
        c = pltpu.make_async_copy(q_hbm.at[:, pl.ds(first, group), :], qg.at[kv, me], qload_sem.at[kv])
        c.start()
        q_loads.append(c)
    kv_loads = []
    for kv in range(kv_local):
        ck = pltpu.make_async_copy(k_hbm.at[:, kv], kbuf.at[kv], kv_sem.at[0, kv])
        cv = pltpu.make_async_copy(v_hbm.at[:, kv], vbuf.at[kv], kv_sem.at[1, kv])
        ck.start()
        cv.start()
        kv_loads.append((ck, cv))

    barrier = pltpu.get_barrier_semaphore()
    for off in range(1, n):
        pl.semaphore_signal(barrier, inc=1, device_id={"seq": lax.rem(me + off, n)}, device_id_type=MESH)
    for c in q_loads:
        c.wait()
    pl.semaphore_wait(barrier, n - 1)

    q_sends = []
    for kv in range(kv_local):
        for off in range(1, n):
            c = pltpu.make_async_remote_copy(
                src_ref=qg.at[kv, me],
                dst_ref=qg.at[kv, me],
                send_sem=qsend_sem.at[kv, off],
                recv_sem=qrecv_sem.at[kv, off],
                device_id={"seq": lax.rem(me + off, n)},
                device_id_type=MESH,
            )
            c.start()
            q_sends.append(c)

    for c in table_loads:
        c.wait()
    page_ids = lax.broadcasted_iota(jnp.int32, (pool, LANES), 0)
    lane = lax.broadcasted_iota(jnp.int32, (1, LANES), 1)

    def match(b, acc):
        length = lens[b]
        for at in range(0, slots, LANES):
            own = owner[at // LANES, pl.ds(b, 1), :]
            loc = local[at // LANES, pl.ds(b, 1), :]
            fill = jnp.clip(length - (lane + at) * page_len, 0, page_len)
            code = jnp.where((own == me) & (fill > 0), loc, -1)
            acc = jnp.where(page_ids == code, (b << bits) + fill, acc)
        return acc

    acc = lax.fori_loop(0, seqs, match, jnp.zeros((pool, LANES), jnp.int32), unroll=8)
    code = jnp.max(acc.astype(jnp.float32), axis=1, keepdims=True)
    wide = jnp.broadcast_to(code, (pool, pool))
    tall = jnp.transpose(wide)[:seqs].astype(jnp.int32)
    wide = wide.astype(jnp.int32)
    full = jnp.broadcast_to(code, (pool, LANES))
    for g in range(group):
        fills[pl.ds(g, pool, stride=group), :] = full
    for at in range(pool * group // LANES):
        codes[at] = jnp.transpose(fills[at * LANES : (at + 1) * LANES, :])[:8].astype(jnp.int32)
    seq_wide = wide[:, :seqs]
    onehot[...] = jnp.where(
        (seq_wide > 0) & ((seq_wide >> bits) == lax.broadcasted_iota(jnp.int32, (pool, seqs), 1)), 1.0, 0.0
    ).astype(jnp.bfloat16)
    spread[...] = jnp.where(
        (tall > 0) & ((tall >> bits) == lax.broadcasted_iota(jnp.int32, (seqs, pool), 0)), 1.0, 0.0
    ).astype(jnp.bfloat16)

    pages_in = LANES // group
    token = lax.broadcasted_iota(jnp.int32, (page_len, LANES), 0)
    lane_page = lax.broadcasted_iota(jnp.int32, (page_len, LANES), 1) // group
    seq_ids = lax.broadcasted_iota(jnp.int32, (seqs, LANES), 0)
    fold_in = lax.broadcasted_iota(jnp.int32, (LANES, LANES), 0)
    fold_out = lax.broadcasted_iota(jnp.int32, (LANES, LANES), 1)
    fold = jnp.where((fold_in % group == fold_out % group) & (fold_out < 2 * group), 1.0, 0.0).astype(jnp.bfloat16)

    def split(value):
        high = value.astype(jnp.bfloat16)
        return high, (value - high.astype(jnp.float32)).astype(jnp.bfloat16)

    def recv(sem, kv, off, ref):
        src = lax.rem(me + n - off, n)
        return pltpu.make_async_remote_copy(
            src_ref=ref.at[kv, src], dst_ref=ref.at[kv, src], send_sem=qsend_sem.at[kv, off],
            recv_sem=sem.at[kv, off], device_id={"seq": src}, device_id_type=MESH,
        )

    o_sends = []
    for kv in range(kv_local):
        for off in range(1, n):
            recv(qrecv_sem, kv, off, qg).wait_recv()
        qf[...] = qg[kv].reshape(seqs * group, dim).astype(jnp.float32)
        for g in range(group):
            mine = qf[pl.ds(g, seqs, stride=group), :].astype(jnp.bfloat16)
            qp[pl.ds(g, pool, stride=group), :] = jnp.dot(
                onehot[...], mine, preferred_element_type=jnp.float32
            )
        for c in kv_loads[kv]:
            c.wait()

        def attend(step, sums):
            rows_at = pl.ds(pl.multiple_of(step * LANES, LANES), LANES)
            q = qp[rows_at, :].astype(jnp.bfloat16)
            k = kbuf[kv, pl.ds(step * pages_in, pages_in)].reshape(pages_in * page_len, dim)
            cross = lax.dot_general(k, q, (((1,), (1,)), ((), ())), preferred_element_type=jnp.float32)
            s = cross[:page_len]
            for j in range(1, pages_in):
                s = jnp.where(lane_page == j, cross[j * page_len : (j + 1) * page_len], s)
            code = codes[step]
            fill = code[:1] & ((1 << bits) - 1)
            w = jnp.where(token < fill, jnp.exp(s * scale - score_shift), 0.0)
            total = jnp.sum(w, axis=0, keepdims=True)
            sums += jnp.where((code[:1] >> bits) == seq_ids, total, 0.0)
            block = jnp.concatenate([jnp.where(lane_page % QUAD == j, w, 0.0) for j in range(QUAD)], axis=0)
            block = jnp.transpose(block).astype(jnp.bfloat16)
            part = QUAD * group
            for j in range(pages_in // QUAD):
                v = vbuf[kv, pl.ds(step * pages_in + j * QUAD, QUAD)].reshape(QUAD * page_len, dim)
                pages[pl.ds(pl.multiple_of(step * LANES + j * part, part), part), :] = jnp.dot(
                    block[j * part : (j + 1) * part], v, preferred_element_type=jnp.float32
                )
            return sums

        sums = lax.fori_loop(0, pool // pages_in, attend, jnp.zeros((seqs, LANES), jnp.float32))
        high, low = split(sums)
        tot = jnp.dot(high, fold, preferred_element_type=jnp.float32) + jnp.dot(
            low, fold, preferred_element_type=jnp.float32
        )

        def collect(value):
            high, low = split(value)
            return jnp.dot(spread[...], high, preferred_element_type=jnp.float32) + jnp.dot(
                spread[...], low, preferred_element_type=jnp.float32
            )

        high = tot.astype(jnp.bfloat16).astype(jnp.float32)
        lanes = lax.broadcasted_iota(jnp.int32, (seqs, LANES), 1)
        tot = jnp.where(lanes < group, high, tot - high)
        for d in range(n):
            stage[kv, d, group * rows : (group + 1) * rows, :] = tot[d * rows : (d + 1) * rows]
        for g in range(group):
            num = collect(pages[pl.ds(g, pool, stride=group), :])
            for d in range(n):
                stage[kv, d, g * rows : (g + 1) * rows, :] = num[d * rows : (d + 1) * rows]
        for d in range(n):
            sbuf[kv, d] = stage[kv, d].astype(jnp.bfloat16)
        for off in range(1, n):
            peer = lax.rem(me + off, n)
            c = pltpu.make_async_remote_copy(
                src_ref=sbuf.at[kv, peer],
                dst_ref=rbuf.at[kv, me],
                send_sem=osend_sem.at[kv, off],
                recv_sem=orecv_sem.at[kv, off],
                device_id={"seq": peer},
                device_id_type=MESH,
            )
            c.start()
            o_sends.append(c)

    for kv in range(kv_local):
        whole = stage[kv, me]
        for off in range(1, n):
            recv(orecv_sem, kv, off, rbuf).wait_recv()
            whole += rbuf[kv, lax.rem(me + n - off, n)].astype(jnp.float32)
        tot = whole[group * rows :]
        for g in range(group):
            den = tot[:, g : g + 1] + tot[:, group + g : group + g + 1]
            outf[pl.ds(kv * group + g, rows, stride=kv_local * group), :] = whole[g * rows : (g + 1) * rows] / den
    out_ref[...] = outf[...].reshape(rows, kv_local * group, dim).astype(jnp.bfloat16)
    for c in q_sends:
        c.wait_send()
    for c in o_sends:
        c.wait_send()


def solution(mesh):
    n = mesh.shape["seq"]

    def body(queries, key_pages, value_pages, page_owner, page_local, seq_lengths):
        pool, kv_local, page_len, dim = key_pages.shape
        seqs, slots = page_owner.shape
        group = HQ // KVH
        rows = seqs // n
        heads = kv_local * group
        part = (group + 1) * rows
        bf16, f32 = jnp.bfloat16, jnp.float32
        in_hbm = pl.BlockSpec(memory_space=pltpu.HBM)
        return pl.pallas_call(
            functools.partial(kernel, n),
            out_shape=jax.ShapeDtypeStruct((rows, heads, dim), bf16),
            in_specs=[in_hbm] * 5 + [pl.BlockSpec(memory_space=pltpu.SMEM)],
            out_specs=pl.BlockSpec(memory_space=pltpu.VMEM),
            scratch_shapes=[
                pltpu.VMEM((kv_local, pool, page_len, dim), bf16),
                pltpu.VMEM((kv_local, pool, page_len, dim), bf16),
                pltpu.VMEM((slots // LANES, seqs, LANES), jnp.int32),
                pltpu.VMEM((slots // LANES, seqs, LANES), jnp.int32),
                pltpu.VMEM((kv_local, n, rows, group, dim), bf16),
                pltpu.VMEM((seqs * group, dim), f32),
                pltpu.VMEM((pool * group, dim), f32),
                pltpu.VMEM((pool * group, LANES), f32),
                pltpu.VMEM((pool * group // LANES, 8, LANES), jnp.int32),
                pltpu.VMEM((pool, seqs), bf16),
                pltpu.VMEM((seqs, pool), bf16),
                pltpu.VMEM((pool * group, dim), f32),
                pltpu.VMEM((kv_local, n, part, dim), f32),
                pltpu.VMEM((kv_local, n, part, dim), bf16),
                pltpu.VMEM((kv_local, n, part, dim), bf16),
                pltpu.VMEM((rows * heads, dim), f32),
                pltpu.SemaphoreType.DMA((2, slots // LANES)),
                pltpu.SemaphoreType.DMA((kv_local,)),
                pltpu.SemaphoreType.DMA((2, kv_local)),
                pltpu.SemaphoreType.DMA((kv_local, n)),
                pltpu.SemaphoreType.DMA((kv_local, n)),
                pltpu.SemaphoreType.DMA((kv_local, n)),
                pltpu.SemaphoreType.DMA((kv_local, n)),
            ],
            compiler_params=pltpu.CompilerParams(
                collective_id=0, has_side_effects=True, vmem_limit_bytes=67043328
            ),
        )(queries, key_pages, value_pages, page_owner, page_local, seq_lengths)

    placed = (
        P(("rep", "seq"), None, None),
        P(("rep", "seq"), "tp", None, None),
        P(("rep", "seq"), "tp", None, None),
        P("rep", None),
        P("rep", None),
        P("rep"),
    )
    return jax.shard_map(
        body, mesh=mesh, in_specs=placed, out_specs=P(("rep", "seq"), "tp", None), check_vma=False
    )
```

```python
import functools
import math

import jax
import jax.numpy as jnp
from jax import lax
from jax.experimental import pallas as pl
from jax.experimental.pallas import tpu as pltpu
from jax.sharding import PartitionSpec as P

HQ = 64
KVH = 8
LANES = 128
QUAD = 4
MESH = pl.DeviceIdType.MESH

score_shift = 8.0


def kernel(
    n, q_hbm, k_hbm, v_hbm, owner_hbm, local_hbm, lens, out_ref,
    kbuf, vbuf, owner, local, qg, qf, qp, fills, codes, onehot, spread, pages, stage, sbuf, rbuf, outf,
    load_sem, qload_sem, kv_sem, qsend_sem, qrecv_sem, osend_sem, orecv_sem,
):
    me = lax.axis_index("seq")
    tp = lax.axis_index("tp")
    pool, kv_local, page_len, dim = k_hbm.shape
    seqs, slots = owner_hbm.shape
    group = HQ // KVH
    rows = seqs // n
    bits = page_len.bit_length()
    scale = 1.0 / math.sqrt(dim)

    table_loads = []
    for at in range(0, slots, LANES):
        part = at // LANES
        for i, (src, dst) in enumerate(((owner_hbm, owner), (local_hbm, local))):
            c = pltpu.make_async_copy(src.at[:, pl.ds(at, LANES)], dst.at[part], load_sem.at[i, part])
            c.start()
            table_loads.append(c)
    q_loads = []
    for kv in range(kv_local):
        first = pl.multiple_of((tp * kv_local + kv) * group, group)
        c = pltpu.make_async_copy(q_hbm.at[:, pl.ds(first, group), :], qg.at[kv, me], qload_sem.at[kv])
        c.start()
        q_loads.append(c)
    kv_loads = []
    for kv in range(kv_local):
        ck = pltpu.make_async_copy(k_hbm.at[:, kv], kbuf.at[kv], kv_sem.at[0, kv])
        cv = pltpu.make_async_copy(v_hbm.at[:, kv], vbuf.at[kv], kv_sem.at[1, kv])
        ck.start()
        cv.start()
        kv_loads.append((ck, cv))

    barrier = pltpu.get_barrier_semaphore()
    for off in range(1, n):
        pl.semaphore_signal(barrier, inc=1, device_id={"seq": lax.rem(me + off, n)}, device_id_type=MESH)
    for c in q_loads:
        c.wait()
    pl.semaphore_wait(barrier, n - 1)

    q_sends = []
    for kv in range(kv_local):
        for off in range(1, n):
            c = pltpu.make_async_remote_copy(
                src_ref=qg.at[kv, me],
                dst_ref=qg.at[kv, me],
                send_sem=qsend_sem.at[kv, off],
                recv_sem=qrecv_sem.at[kv, off],
                device_id={"seq": lax.rem(me + off, n)},
                device_id_type=MESH,
            )
            c.start()
            q_sends.append(c)

    for c in table_loads:
        c.wait()
    page_ids = lax.broadcasted_iota(jnp.int32, (pool, LANES), 0)
    lane = lax.broadcasted_iota(jnp.int32, (1, LANES), 1)

    def match(b, acc):
        length = lens[b]
        for at in range(0, slots, LANES):
            own = owner[at // LANES, pl.ds(b, 1), :]
            loc = local[at // LANES, pl.ds(b, 1), :]
            fill = jnp.clip(length - (lane + at) * page_len, 0, page_len)
            code = jnp.where((own == me) & (fill > 0), loc, -1)
            acc = jnp.where(page_ids == code, (b << bits) + fill, acc)
        return acc

    acc = lax.fori_loop(0, seqs, match, jnp.zeros((pool, LANES), jnp.int32), unroll=8)
    code = jnp.max(acc.astype(jnp.float32), axis=1, keepdims=True)
    wide = jnp.broadcast_to(code, (pool, pool))
    tall = jnp.transpose(wide)[:seqs].astype(jnp.int32)
    wide = wide.astype(jnp.int32)
    full = jnp.broadcast_to(code, (pool, LANES))
    for g in range(group):
        fills[pl.ds(g, pool, stride=group), :] = full
    for at in range(pool * group // LANES):
        codes[at] = jnp.transpose(fills[at * LANES : (at + 1) * LANES, :])[:8].astype(jnp.int32)
    seq_wide = wide[:, :seqs]
    onehot[...] = jnp.where(
        (seq_wide > 0) & ((seq_wide >> bits) == lax.broadcasted_iota(jnp.int32, (pool, seqs), 1)), 1.0, 0.0
    ).astype(jnp.bfloat16)
    spread[...] = jnp.where(
        (tall > 0) & ((tall >> bits) == lax.broadcasted_iota(jnp.int32, (seqs, pool), 0)), 1.0, 0.0
    ).astype(jnp.bfloat16)

    pages_in = LANES // group
    token = lax.broadcasted_iota(jnp.int32, (page_len, LANES), 0)
    lane_page = lax.broadcasted_iota(jnp.int32, (page_len, LANES), 1) // group
    seq_ids = lax.broadcasted_iota(jnp.int32, (seqs, LANES), 0)
    fold_in = lax.broadcasted_iota(jnp.int32, (LANES, LANES), 0)
    fold_out = lax.broadcasted_iota(jnp.int32, (LANES, LANES), 1)
    fold = jnp.where((fold_in % group == fold_out % group) & (fold_out < 2 * group), 1.0, 0.0).astype(jnp.bfloat16)

    def split(value):
        high = value.astype(jnp.bfloat16)
        return high, (value - high.astype(jnp.float32)).astype(jnp.bfloat16)

    def recv(sem, kv, off, ref):
        src = lax.rem(me + n - off, n)
        return pltpu.make_async_remote_copy(
            src_ref=ref.at[kv, src], dst_ref=ref.at[kv, src], send_sem=qsend_sem.at[kv, off],
            recv_sem=sem.at[kv, off], device_id={"seq": src}, device_id_type=MESH,
        )

    o_sends = []
    for kv in range(kv_local):
        for off in range(1, n):
            recv(qrecv_sem, kv, off, qg).wait_recv()
        qf[...] = qg[kv].reshape(seqs * group, dim).astype(jnp.float32)
        for g in range(group):
            mine = qf[pl.ds(g, seqs, stride=group), :].astype(jnp.bfloat16)
            qp[pl.ds(g, pool, stride=group), :] = jnp.dot(
                onehot[...], mine, preferred_element_type=jnp.float32
            )
        for c in kv_loads[kv]:
            c.wait()

        def attend(step, sums):
            rows_at = pl.ds(pl.multiple_of(step * LANES, LANES), LANES)
            q = qp[rows_at, :].astype(jnp.bfloat16)
            k = kbuf[kv, pl.ds(step * pages_in, pages_in)].reshape(pages_in * page_len, dim)
            cross = lax.dot_general(k, q, (((1,), (1,)), ((), ())), preferred_element_type=jnp.float32)
            s = cross[:page_len]
            for j in range(1, pages_in):
                s = jnp.where(lane_page == j, cross[j * page_len : (j + 1) * page_len], s)
            code = codes[step]
            fill = code[:1] & ((1 << bits) - 1)
            w = jnp.where(token < fill, jnp.exp(s * scale - score_shift), 0.0)
            total = jnp.sum(w, axis=0, keepdims=True)
            sums += jnp.where((code[:1] >> bits) == seq_ids, total, 0.0)
            block = jnp.concatenate([jnp.where(lane_page % QUAD == j, w, 0.0) for j in range(QUAD)], axis=0)
            block = jnp.transpose(block).astype(jnp.bfloat16)
            part = QUAD * group
            for j in range(pages_in // QUAD):
                v = vbuf[kv, pl.ds(step * pages_in + j * QUAD, QUAD)].reshape(QUAD * page_len, dim)
                pages[pl.ds(pl.multiple_of(step * LANES + j * part, part), part), :] = jnp.dot(
                    block[j * part : (j + 1) * part], v, preferred_element_type=jnp.float32
                )
            return sums

        sums = lax.fori_loop(0, pool // pages_in, attend, jnp.zeros((seqs, LANES), jnp.float32), unroll=2)
        high, low = split(sums)
        tot = jnp.dot(high, fold, preferred_element_type=jnp.float32) + jnp.dot(
            low, fold, preferred_element_type=jnp.float32
        )

        def collect(value):
            high, low = split(value)
            return jnp.dot(spread[...], high, preferred_element_type=jnp.float32) + jnp.dot(
                spread[...], low, preferred_element_type=jnp.float32
            )

        high = tot.astype(jnp.bfloat16).astype(jnp.float32)
        lanes = lax.broadcasted_iota(jnp.int32, (seqs, LANES), 1)
        tot = jnp.where(lanes < group, high, tot - high)
        for d in range(n):
            stage[kv, d, group * rows : (group + 1) * rows, :] = tot[d * rows : (d + 1) * rows]
        for g in range(group):
            num = collect(pages[pl.ds(g, pool, stride=group), :])
            for d in range(n):
                stage[kv, d, g * rows : (g + 1) * rows, :] = num[d * rows : (d + 1) * rows]
        for d in range(n):
            sbuf[kv, d] = stage[kv, d].astype(jnp.bfloat16)
        for off in range(1, n):
            peer = lax.rem(me + off, n)
            c = pltpu.make_async_remote_copy(
                src_ref=sbuf.at[kv, peer],
                dst_ref=rbuf.at[kv, me],
                send_sem=osend_sem.at[kv, off],
                recv_sem=orecv_sem.at[kv, off],
                device_id={"seq": peer},
                device_id_type=MESH,
            )
            c.start()
            o_sends.append(c)

    for kv in range(kv_local):
        whole = stage[kv, me]
        for off in range(1, n):
            recv(orecv_sem, kv, off, rbuf).wait_recv()
            whole += rbuf[kv, lax.rem(me + n - off, n)].astype(jnp.float32)
        tot = whole[group * rows :]
        for g in range(group):
            den = tot[:, g : g + 1] + tot[:, group + g : group + g + 1]
            outf[pl.ds(kv * group + g, rows, stride=kv_local * group), :] = whole[g * rows : (g + 1) * rows] / den
    out_ref[...] = outf[...].reshape(rows, kv_local * group, dim).astype(jnp.bfloat16)
    for c in q_sends:
        c.wait_send()
    for c in o_sends:
        c.wait_send()


def solution(mesh):
    n = mesh.shape["seq"]

    def body(queries, key_pages, value_pages, page_owner, page_local, seq_lengths):
        pool, kv_local, page_len, dim = key_pages.shape
        seqs, slots = page_owner.shape
        group = HQ // KVH
        rows = seqs // n
        heads = kv_local * group
        part = (group + 1) * rows
        bf16, f32 = jnp.bfloat16, jnp.float32
        in_hbm = pl.BlockSpec(memory_space=pltpu.HBM)
        return pl.pallas_call(
            functools.partial(kernel, n),
            out_shape=jax.ShapeDtypeStruct((rows, heads, dim), bf16),
            in_specs=[in_hbm] * 5 + [pl.BlockSpec(memory_space=pltpu.SMEM)],
            out_specs=pl.BlockSpec(memory_space=pltpu.VMEM),
            scratch_shapes=[
                pltpu.VMEM((kv_local, pool, page_len, dim), bf16),
                pltpu.VMEM((kv_local, pool, page_len, dim), bf16),
                pltpu.VMEM((slots // LANES, seqs, LANES), jnp.int32),
                pltpu.VMEM((slots // LANES, seqs, LANES), jnp.int32),
                pltpu.VMEM((kv_local, n, rows, group, dim), bf16),
                pltpu.VMEM((seqs * group, dim), f32),
                pltpu.VMEM((pool * group, dim), f32),
                pltpu.VMEM((pool * group, LANES), f32),
                pltpu.VMEM((pool * group // LANES, 8, LANES), jnp.int32),
                pltpu.VMEM((pool, seqs), bf16),
                pltpu.VMEM((seqs, pool), bf16),
                pltpu.VMEM((pool * group, dim), f32),
                pltpu.VMEM((kv_local, n, part, dim), f32),
                pltpu.VMEM((kv_local, n, part, dim), bf16),
                pltpu.VMEM((kv_local, n, part, dim), bf16),
                pltpu.VMEM((rows * heads, dim), f32),
                pltpu.SemaphoreType.DMA((2, slots // LANES)),
                pltpu.SemaphoreType.DMA((kv_local,)),
                pltpu.SemaphoreType.DMA((2, kv_local)),
                pltpu.SemaphoreType.DMA((kv_local, n)),
                pltpu.SemaphoreType.DMA((kv_local, n)),
                pltpu.SemaphoreType.DMA((kv_local, n)),
                pltpu.SemaphoreType.DMA((kv_local, n)),
            ],
            compiler_params=pltpu.CompilerParams(
                collective_id=0, has_side_effects=True, vmem_limit_bytes=67043328
            ),
        )(queries, key_pages, value_pages, page_owner, page_local, seq_lengths)

    placed = (
        P(("rep", "seq"), None, None),
        P(("rep", "seq"), "tp", None, None),
        P(("rep", "seq"), "tp", None, None),
        P("rep", None),
        P("rep", None),
        P("rep"),
    )
    return jax.shard_map(
        body, mesh=mesh, in_specs=placed, out_specs=P(("rep", "seq"), "tp", None), check_vma=False
    )
```
